32 devices in a mesh: rows: 8 (over z, y), cols: 4 (over x, core).
Axes of the slice: x: 2, y: 2, z: 4, core: 2. Of those that a mesh axis runs over, the one named last changes fastest.
Arguments:
- adjacency_tiles: bfloat16 [192, 12, 128, 128], P(('rows', 'cols')), may hold values from 2.170139e-08 to 0.25
- col_block: int32 [192, 12], P(('rows', 'cols')), may hold values from 0 to 191, as said below
- label_prior: float32 [24576, 256], P(('rows', 'cols')), may hold values from 0.05 to 20.1
- seed_label: int32 [24576], P(('rows', 'cols')), may hold values from 0 to 255
- seed_mask: int32 [24576], P(('rows', 'cols')), may hold values 0 or 1
Outputs:
- labels: float32 [24576, 256], P(('rows', 'cols'))
The draws below stay inside these ranges and needn't reach their ends.
Inputs may be any that keep to these rules, and one draw needn't show every extreme that they name: Row block b is held by device b // 6 of rows+cols, whose rows group is b // (6 * 4). col_block[b, 0] = b. For each device, all its tiles that reference blocks of another rows group reference one and the same block of that group, and each device references every rows group.
All inputs are finite; a program needn't handle non-finite values. No bound on the sum of `seed_mask` on one device may be relied on, other than what follows from the above.
Results may differ from the reference program's by a relative error of at most 0.00041.
Values may be sent and summed in bfloat16 or wider, within the bound.
A program may use at most 64 MiB of HBM per device.

```python
import jax
import jax.numpy as jnp
from jax import lax

CLASSES = 256
BLOCK = 128
DEGREE = 12
HOPS = 4
BLOCKS_DEV = 6
BLOCKS = 192
NODES = 24576
N_ROWS = 8
N_COLS = 4


def draw_col_block(key, part):
    device_count = BLOCKS // BLOCKS_DEV
    group_size = N_COLS * BLOCKS_DEV
    slot_count = BLOCKS_DEV * (DEGREE - 1)

    def per_device(device):
        device_key = jax.random.fold_in(jax.random.fold_in(key, 7177), device)
        k_within, k_group, k_local, k_coin, k_perm = jax.random.split(device_key, 5)
        home_group = device // N_COLS
        chosen = jax.random.randint(k_within, (N_ROWS,), 0, group_size)
        extra_group = jax.random.randint(k_group, (slot_count - N_ROWS,), 0, N_ROWS)
        coin_flip = jax.random.randint(k_coin, (slot_count - N_ROWS,), 0, 2)
        extra_group = jnp.where(coin_flip == 0, home_group, extra_group)
        groups_all = jnp.concatenate([jnp.arange(N_ROWS, dtype=jnp.int32), extra_group.astype(jnp.int32)])
        local_pick = jax.random.randint(k_local, (slot_count,), 0, group_size)
        within_all = jnp.where(groups_all == home_group, local_pick, chosen[groups_all])
        shuffle = jax.random.permutation(k_perm, slot_count)
        picked = (groups_all * group_size + within_all)[shuffle].reshape(BLOCKS_DEV, DEGREE - 1)
        diagonal = device * BLOCKS_DEV + jnp.arange(BLOCKS_DEV, dtype=jnp.int32)
        return jnp.concatenate([diagonal[:, None], picked.astype(jnp.int32)], axis=1)
    result = jax.vmap(per_device)(jnp.arange(device_count, dtype=jnp.int32))
    return result.reshape(BLOCKS, DEGREE).astype(jnp.int32)


def draw_adjacency_tiles(key, part):
    k_scale, k_entry, k_pick = jax.random.split(jax.random.fold_in(key, 3301), 3)
    span = jnp.log(jnp.float32(100.0))
    tile_scale = jnp.exp(span * jax.random.uniform(k_scale, (BLOCKS, DEGREE), jnp.float32))
    tile_scale = tile_scale / jnp.sum(tile_scale, axis=1, keepdims=True)
    shape = (BLOCKS, DEGREE, BLOCK, BLOCK)
    entries = jnp.exp(jax.random.uniform(k_entry, shape, jnp.float32, jnp.log(0.5), jnp.log(2.0)))
    dominant = jax.random.randint(k_pick, shape, 0, 16) == 0
    pattern = jnp.where(dominant, entries * (16.0 / BLOCK), jnp.float32(0.01 / BLOCK))
    values = tile_scale[:, :, None, None] * pattern
    return values.astype(jnp.bfloat16)


def draw_label_prior(key, part):
    k_base, k_pick, k_boost = jax.random.split(jax.random.fold_in(key, 5407), 3)
    base = jnp.exp(jax.random.uniform(k_base, (NODES, CLASSES), jnp.float32, jnp.log(0.05), 0.0))
    picked = jax.random.randint(k_pick, (NODES, CLASSES), 0, 16) == 0
    boost = jnp.exp(3.0 * jax.random.uniform(k_boost, (NODES, CLASSES), jnp.float32))
    factor = jnp.where(picked, boost, jnp.float32(1.0))
    return (base * factor).astype(jnp.float32)


def with_ends(values, rng, low, high):
    spot = [jax.random.randint(jax.random.fold_in(rng, axis), (), 0, length) for axis, length in enumerate(values.shape)]
    main_axis = values.shape.index(max(values.shape))
    beside = spot[:main_axis] + [(spot[main_axis] + 1) % values.shape[main_axis]] + spot[main_axis + 1:]
    return values.at[tuple(spot)].set(low).at[tuple(beside)].set(high)


def setup_inputs(seed: int = 0) -> dict:
    seeds = jax.random.split(jax.random.key(seed), 6)
    adjacency_tiles = draw_adjacency_tiles(jax.random.fold_in(seeds[5], 71), 0)
    col_block = draw_col_block(jax.random.fold_in(seeds[5], 71), 0)
    label_prior = draw_label_prior(jax.random.fold_in(seeds[5], 71), 0)
    seed_label = with_ends(jax.random.randint(seeds[3], (NODES,), 0, CLASSES), jax.random.fold_in(seeds[3], 1), 0, CLASSES - 1).astype(jnp.int32)
    seed_mask = with_ends((jax.random.randint(seeds[4], (NODES,), 0, 4) < 1).astype(jnp.int32), jax.random.fold_in(seeds[4], 1), 0, 1)
    return {"adjacency_tiles": adjacency_tiles, "col_block": col_block, "label_prior": label_prior, "seed_label": seed_label, "seed_mask": seed_mask}


ALPHA = 0.85
SEED_BOOST = 8.0


def prepare(label_prior, seed_label, seed_mask):
    classes = label_prior.shape[1]
    one_hot = (seed_label[:, None] == jnp.arange(classes, dtype=jnp.int32)[None, :]).astype(jnp.float32)
    anchor_raw = label_prior + SEED_BOOST * seed_mask[:, None].astype(jnp.float32) * one_hot
    return anchor_raw * (classes / jnp.sum(anchor_raw, axis=1, keepdims=True))


def reference(adjacency_tiles, col_block, label_prior, seed_label, seed_mask):
    anchor = prepare(label_prior, seed_label, seed_mask)
    labels = anchor
    for hop_index in range(HOPS):
        sent_blocks = labels.astype(jnp.bfloat16).reshape(BLOCKS, BLOCK, CLASSES)

        def per_block(pair_in):
            tile_set, col_ids = pair_in
            operand = sent_blocks[col_ids]
            return jnp.einsum("kij,kjc->ic", tile_set.astype(jnp.float32), operand.astype(jnp.float32))

        spread = lax.map(per_block, (adjacency_tiles, col_block), batch_size=16).reshape(NODES, CLASSES)
        blended = ALPHA * spread + (1.0 - ALPHA) * anchor
        labels = blended * (CLASSES / jnp.sum(blended, axis=1, keepdims=True))
    return labels
```

```python
import functools

import jax
import jax.numpy as jnp
from jax import lax
from jax.experimental import pallas as pl
from jax.experimental.pallas import tpu as pltpu
from jax.sharding import PartitionSpec as P

HOPS = 4
CHUNKS = 4
ALPHA = 0.85
SEED_BOOST = 8.0
LANES = 128
MESH = pl.DeviceIdType.MESH


def prepare(label_prior, seed_label, seed_mask):
    classes = label_prior.shape[1]
    one_hot = (seed_label[:, None] == jnp.arange(classes, dtype=jnp.int32)[None, :]).astype(
        jnp.float32
    )
    anchor_raw = label_prior + SEED_BOOST * seed_mask[:, None].astype(jnp.float32) * one_hot
    return anchor_raw * (classes / jnp.sum(anchor_raw, axis=1, keepdims=True))


def kernel(
    n_rows, n_cols, blocks_dev, degree, block_rows, classes,
    index_ref, wanted_ref, anchor_ref, adj_hbm, out_ref,
    tables, remote, reply, adj, asked_v, asked_s,
    adj_sem, asked_send, asked_recv, asked_copy,
    near_send, near_recv, far_send, far_recv, fwd_send, fwd_recv, rep_send, rep_recv,
):
    row = lax.axis_index("rows")
    col = lax.axis_index("cols")
    group = n_cols * blocks_dev
    width = 2 if n_cols % 2 == 0 else 1
    pairs = n_cols // width
    pair, low = col // width, col % width
    mate = pair * width + (width - 1 - low)
    chunk = block_rows // CHUNKS
    peers = n_rows - 1

    def far_col(j):
        return ((pair + j) % pairs) * width + low

    def from_col(j):
        return ((pair + pairs - j) % pairs) * width + low

    def each_peer(body):
        half = n_rows // 2
        def step(i):
            if isinstance(i, int):
                d = half + ((i + 1) // 2) * (1 - 2 * (i % 2))
            else:
                d = half + lax.div(i + 1, 2) * (1 - 2 * lax.rem(i, 2))
            body((row + d + n_rows) % n_rows)
        if n_rows <= 8:
            for i in range(peers):
                step(i)
        else:
            def loop(i, carry):
                step(i)
                return carry
            lax.fori_loop(0, peers, loop, 0)

    adj_copy = pltpu.make_async_copy(adj_hbm, adj, adj_sem)
    adj_copy.start()

    barrier = pltpu.get_barrier_semaphore()
    greeted = peers
    if width == 2:
        pl.semaphore_signal(barrier, inc=1, device_id=(row, mate), device_id_type=MESH)
        greeted += 1
    for j in range(1, pairs):
        pl.semaphore_signal(barrier, inc=1, device_id=(row, far_col(j)), device_id_type=MESH)
        greeted += 1
    each_peer(
        lambda other: pl.semaphore_signal(
            barrier, inc=1, device_id=(other, col), device_id_type=MESH
        )
    )
    def keep(p, b, labels):
        sent = labels.astype(jnp.bfloat16)
        for q in range(CHUNKS):
            tables[p][q][col * blocks_dev + b] = sent[q * chunk : (q + 1) * chunk, :]

    for b in range(blocks_dev):
        keep(0, b, anchor_ref[b * block_rows : (b + 1) * block_rows, :])
    pl.semaphore_wait(barrier, greeted)

    def part(p, owner, q):
        return tables[p][q].at[pl.ds(owner * blocks_dev, blocks_dev)]

    def near(p, q):
        ref = part(p, col, q)
        return pltpu.make_async_remote_copy(
            src_ref=ref, dst_ref=ref, send_sem=near_send.at[p, q], recv_sem=near_recv.at[p, q],
            device_id=(row, mate), device_id_type=MESH,
        )

    def far(p, j, q):
        ref = part(p, col, q)
        return pltpu.make_async_remote_copy(
            src_ref=ref, dst_ref=ref,
            send_sem=far_send.at[p, j - 1, q], recv_sem=far_recv.at[p, j - 1, q],
            device_id=(row, far_col(j)), device_id_type=MESH,
        )

    def forward(p, j, q):
        ref = part(p, from_col(j), q)
        return pltpu.make_async_remote_copy(
            src_ref=ref, dst_ref=ref,
            send_sem=fwd_send.at[p, j - 1, q], recv_sem=fwd_recv.at[p, j - 1, q],
            device_id=(row, mate), device_id_type=MESH,
        )

    def start_gather(p):
        for q in range(CHUNKS):
            for j in range(1, pairs):
                far(p, j, q).start()
            if width == 2:
                near(p, q).start()

    start_gather(0)

    def send_wanted(other):
        pltpu.make_async_remote_copy(
            src_ref=wanted_ref, dst_ref=asked_v.at[row], send_sem=asked_send, recv_sem=asked_recv,
            device_id=(other, col), device_id_type=MESH,
        ).start()

    each_peer(send_wanted)
    all_asked = asked_v.at[pl.ds(0, peers)]
    pltpu.make_async_copy(all_asked, all_asked, asked_recv).wait()
    pltpu.make_async_copy(all_asked, all_asked, asked_send).wait()
    to_scalar = pltpu.make_async_copy(asked_v, asked_s, asked_copy)
    to_scalar.start()
    to_scalar.wait()
    adj_copy.wait()

    def load(p, b, k):
        index = index_ref[b * degree + k]
        return [tables[p][q][index] for q in range(CHUNKS)]

    def hop(p, last):
        for q in range(CHUNKS):
            rows_q = pl.ds(q * chunk, chunk)
            for j in range(1, pairs):
                far(p, j, q).wait_recv()
                if width == 2:
                    forward(p, j, q).start()
            if width == 2:
                near(p, q).wait_recv()
                for j in range(1, pairs):
                    forward(p, j, q).wait_recv()

            def answer(other):
                reply[other, rows_q, :] = tables[p][q][asked_s[other, 0, row]]
                pltpu.make_async_remote_copy(
                    src_ref=reply.at[other, rows_q, :],
                    dst_ref=remote.at[p, row, rows_q, :],
                    send_sem=rep_send.at[p], recv_sem=rep_recv.at[p],
                    device_id=(other, col), device_id_type=MESH,
                ).start()

            each_peer(answer)
        got = remote.at[p, pl.ds(0, peers)]
        pltpu.make_async_copy(got, got, rep_recv.at[p]).wait()

        def fold(other):
            for q in range(CHUNKS):
                tables[p][q][group + other] = remote[p, other, pl.ds(q * chunk, chunk), :]

        each_peer(fold)

        step = 2 if degree % 2 == 0 else 1
        for b in range(blocks_dev):
            spread = jnp.zeros((block_rows, classes), jnp.float32)
            for k in range(0, degree, step):
                lhs = jnp.concatenate([adj[b, k + i] for i in range(step)], axis=1)
                rhs = jnp.concatenate(sum([load(p, b, k + i) for i in range(step)], []), axis=0)
                spread = spread + jnp.dot(lhs, rhs, preferred_element_type=jnp.float32)
            here = slice(b * block_rows, (b + 1) * block_rows)
            blended = ALPHA * spread + (1.0 - ALPHA) * anchor_ref[here, :]
            labels = blended * (classes / jnp.sum(blended, axis=1, keepdims=True))
            out_ref[here, :] = labels
            keep(1 - p, b, labels)

        for q in range(CHUNKS):
            for j in range(1, pairs):
                far(p, j, q).wait_send()
                if width == 2:
                    forward(p, j, q).wait_send()
            if width == 2:
                near(p, q).wait_send()
        sent = reply.at[pl.ds(0, peers)]
        pltpu.make_async_copy(sent, sent, rep_send.at[p]).wait()

        if not last:
            start_gather(1 - p)

    for h in range(HOPS):
        hop(h % 2, h == HOPS - 1)


def local(adjacency_tiles, col_block, label_prior, seed_label, seed_mask):
    blocks_dev, degree, block_rows, _ = adjacency_tiles.shape
    nodes, classes = label_prior.shape
    n_rows = lax.axis_size("rows")
    n_cols = lax.axis_size("cols")
    group = n_cols * blocks_dev
    own_group = lax.axis_index("rows")
    owner_group = col_block // group
    within = col_block % group
    table_index = jnp.where(owner_group == own_group, within, group + owner_group).reshape(-1)
    padded = -(-n_rows // LANES) * LANES
    group_ids = jnp.arange(padded, dtype=jnp.int32)
    matched = owner_group.reshape(-1)[:, None] == group_ids[None, :]
    wanted = jnp.max(jnp.where(matched, within.reshape(-1)[:, None], 0), axis=0)[None, :]
    anchor = prepare(label_prior, seed_label, seed_mask)
    pairs = max(n_cols // 2 if n_cols % 2 == 0 else n_cols, 2)
    dma = pltpu.SemaphoreType.DMA
    vmem = pl.BlockSpec(memory_space=pltpu.VMEM)
    return pl.pallas_call(
        functools.partial(kernel, n_rows, n_cols, blocks_dev, degree, block_rows, classes),
        out_shape=jax.ShapeDtypeStruct((nodes, classes), jnp.float32),
        in_specs=[
            pl.BlockSpec(memory_space=pltpu.SMEM),
            vmem,
            vmem,
            pl.BlockSpec(memory_space=pl.ANY),
        ],
        out_specs=vmem,
        scratch_shapes=[
            [
                [
                    pltpu.VMEM((group + n_rows, block_rows // CHUNKS, classes), jnp.bfloat16)
                    for _ in range(CHUNKS)
                ]
                for _ in range(2)
            ],
            pltpu.VMEM((2, n_rows, block_rows, classes), jnp.bfloat16),
            pltpu.VMEM((n_rows, block_rows, classes), jnp.bfloat16),
            pltpu.VMEM(adjacency_tiles.shape, jnp.bfloat16),
            pltpu.VMEM((n_rows, 1, padded), jnp.int32),
            pltpu.SMEM((n_rows, 1, padded), jnp.int32),
            dma, dma, dma, dma,
            dma((2, CHUNKS)), dma((2, CHUNKS)),
            dma((2, pairs - 1, CHUNKS)), dma((2, pairs - 1, CHUNKS)),
            dma((2, pairs - 1, CHUNKS)), dma((2, pairs - 1, CHUNKS)),
            dma((2,)), dma((2,)),
        ],
        compiler_params=pltpu.CompilerParams(
            collective_id=0, has_side_effects=True, vmem_limit_bytes=60 * 1024 * 1024
        ),
    )(table_index, wanted, anchor, adjacency_tiles)


def solution(mesh):
    in_specs = (
        P(("rows", "cols"), None, None, None),
        P(("rows", "cols"), None),
        P(("rows", "cols"), None),
        P(("rows", "cols")),
        P(("rows", "cols")),
    )
    out_specs = P(("rows", "cols"), None)
    return jax.shard_map(local, mesh=mesh, in_specs=in_specs, out_specs=out_specs, check_vma=False)
```

```python
import functools

import jax
import jax.numpy as jnp
from jax import lax
from jax.experimental import pallas as pl
from jax.experimental.pallas import tpu as pltpu
from jax.sharding import PartitionSpec as P

HOPS = 4
CHUNK_PARTS = (1, 1, 2, 2, 2)
CHUNKS = len(CHUNK_PARTS)
ALPHA = 0.85
SEED_BOOST = 8.0
LANES = 128
MESH = pl.DeviceIdType.MESH


def kernel(
    n_rows, n_cols, blocks_dev, degree, block_rows, classes,
    col_block_ref, prior_ref, label_ref, mask_ref, adj_hbm, out_ref,
    tables, remote, reply, adj, anchor_ref, index_ref, wanted_ref, asked_v, asked_s,
    adj_sem, asked_send, asked_recv, asked_copy,
    near_send, near_recv, far_send, far_recv, fwd_send, fwd_recv, rep_send, rep_recv,
):
    row = lax.axis_index("rows")
    col = lax.axis_index("cols")
    group = n_cols * blocks_dev
    width = 2 if n_cols % 2 == 0 else 1
    pairs = n_cols // width
    pair, low = col // width, col % width
    mate = pair * width + (width - 1 - low)
    unit = block_rows // sum(CHUNK_PARTS)
    starts = [unit * sum(CHUNK_PARTS[:q]) for q in range(CHUNKS)]
    sizes = [unit * part for part in CHUNK_PARTS]
    peers = n_rows - 1

    def far_col(j):
        return ((pair + j) % pairs) * width + low

    def from_col(j):
        return ((pair + pairs - j) % pairs) * width + low

    def each_peer(body):
        half = n_rows // 2
        def step(i):
            if isinstance(i, int):
                d = half + ((i + 1) // 2) * (1 - 2 * (i % 2))
            else:
                d = half + lax.div(i + 1, 2) * (1 - 2 * lax.rem(i, 2))
            body((row + d + n_rows) % n_rows)
        if n_rows <= 8:
            for i in range(peers):
                step(i)
        else:
            def loop(i, carry):
                step(i)
                return carry
            lax.fori_loop(0, peers, loop, 0)

    adj_copy = pltpu.make_async_copy(adj_hbm, adj, adj_sem)
    adj_copy.start()

    barrier = pltpu.get_barrier_semaphore()
    greeted = peers
    if width == 2:
        pl.semaphore_signal(barrier, inc=1, device_id=(row, mate), device_id_type=MESH)
        greeted += 1
    for j in range(1, pairs):
        pl.semaphore_signal(barrier, inc=1, device_id=(row, far_col(j)), device_id_type=MESH)
        greeted += 1
    each_peer(
        lambda other: pl.semaphore_signal(
            barrier, inc=1, device_id=(other, col), device_id_type=MESH
        )
    )
    def keep(p, b, labels):
        sent = labels.astype(jnp.bfloat16)
        for q in range(CHUNKS):
            tables[p][q][col * blocks_dev + b] = sent[starts[q] : starts[q] + sizes[q], :]

    code = jnp.where(mask_ref[...] > 0, label_ref[...], -1)
    for b in range(blocks_dev):
        here = slice(b * block_rows, (b + 1) * block_rows)
        across = jnp.broadcast_to(code[b : b + 1, :], (block_rows, block_rows)).T
        class_id = lax.broadcasted_iota(jnp.int32, (block_rows, classes), 1)
        across = jnp.concatenate([across] * (classes // block_rows), axis=1)
        raw = prior_ref[here, :] + jnp.where(class_id == across, SEED_BOOST, 0.0)
        anchor = raw * (classes / jnp.sum(raw, axis=1, keepdims=True))
        anchor_ref[here, :] = anchor
        keep(0, b, anchor)
    pl.semaphore_wait(barrier, greeted)

    def part(p, owner, q):
        return tables[p][q].at[pl.ds(owner * blocks_dev, blocks_dev)]

    def near(p, q):
        ref = part(p, col, q)
        return pltpu.make_async_remote_copy(
            src_ref=ref, dst_ref=ref, send_sem=near_send.at[p, q], recv_sem=near_recv.at[p, q],
            device_id=(row, mate), device_id_type=MESH,
        )

    def far(p, j, q):
        ref = part(p, col, q)
        return pltpu.make_async_remote_copy(
            src_ref=ref, dst_ref=ref,
            send_sem=far_send.at[p, j - 1, q], recv_sem=far_recv.at[p, j - 1, q],
            device_id=(row, far_col(j)), device_id_type=MESH,
        )

    def forward(p, j, q):
        ref = part(p, from_col(j), q)
        return pltpu.make_async_remote_copy(
            src_ref=ref, dst_ref=ref,
            send_sem=fwd_send.at[p, j - 1, q], recv_sem=fwd_recv.at[p, j - 1, q],
            device_id=(row, mate), device_id_type=MESH,
        )

    def start_gather(p):
        for q in range(CHUNKS):
            for j in range(1, pairs):
                far(p, j, q).start()
            if width == 2:
                near(p, q).start()

    start_gather(0)

    lane = lax.broadcasted_iota(jnp.int32, wanted_ref.shape, 1)
    wanted = jnp.zeros(wanted_ref.shape, jnp.int32)
    for b in range(blocks_dev):
        for k in range(degree):
            block = col_block_ref[b, k]
            owner = lax.div(block, group)
            within = block - owner * group
            index_ref[b * degree + k] = jnp.where(owner == row, within, group + owner)
            wanted = jnp.where(lane == owner, within, wanted)
    wanted_ref[...] = wanted

    def send_wanted(other):
        pltpu.make_async_remote_copy(
            src_ref=wanted_ref, dst_ref=asked_v.at[row], send_sem=asked_send, recv_sem=asked_recv,
            device_id=(other, col), device_id_type=MESH,
        ).start()

    each_peer(send_wanted)
    all_asked = asked_v.at[pl.ds(0, peers)]
    pltpu.make_async_copy(all_asked, all_asked, asked_recv).wait()
    pltpu.make_async_copy(all_asked, all_asked, asked_send).wait()
    to_scalar = pltpu.make_async_copy(asked_v, asked_s, asked_copy)
    to_scalar.start()
    to_scalar.wait()
    adj_copy.wait()

    def load(p, b, k):
        index = index_ref[b * degree + k]
        return [tables[p][q][index] for q in range(CHUNKS)]

    def hop(p, last):
        for q in range(CHUNKS):
            rows_q = pl.ds(starts[q], sizes[q])
            for j in range(1, pairs):
                far(p, j, q).wait_recv()
                if width == 2:
                    forward(p, j, q).start()
            if width == 2:
                near(p, q).wait_recv()
                for j in range(1, pairs):
                    forward(p, j, q).wait_recv()

            def answer(other):
                reply[other, rows_q, :] = tables[p][q][asked_s[other, 0, row]]
                pltpu.make_async_remote_copy(
                    src_ref=reply.at[other, rows_q, :],
                    dst_ref=remote.at[p, row, rows_q, :],
                    send_sem=rep_send.at[p], recv_sem=rep_recv.at[p],
                    device_id=(other, col), device_id_type=MESH,
                ).start()

            each_peer(answer)
        got = remote.at[p, pl.ds(0, peers)]
        pltpu.make_async_copy(got, got, rep_recv.at[p]).wait()

        def fold(other):
            for q in range(CHUNKS):
                tables[p][q][group + other] = remote[p, other, pl.ds(starts[q], sizes[q]), :]

        each_peer(fold)

        step = 2 if degree % 2 == 0 else 1
        for b in range(blocks_dev):
            spread = jnp.zeros((block_rows, classes), jnp.float32)
            for k in range(0, degree, step):
                lhs = jnp.concatenate([adj[b, k + i] for i in range(step)], axis=1)
                rhs = jnp.concatenate(sum([load(p, b, k + i) for i in range(step)], []), axis=0)
                spread = spread + jnp.dot(lhs, rhs, preferred_element_type=jnp.float32)
            here = slice(b * block_rows, (b + 1) * block_rows)
            blended = ALPHA * spread + (1.0 - ALPHA) * anchor_ref[here, :]
            labels = blended * (classes / jnp.sum(blended, axis=1, keepdims=True))
            out_ref[here, :] = labels
            keep(1 - p, b, labels)

        for q in range(CHUNKS):
            for j in range(1, pairs):
                far(p, j, q).wait_send()
                if width == 2:
                    forward(p, j, q).wait_send()
            if width == 2:
                near(p, q).wait_send()
        sent = reply.at[pl.ds(0, peers)]
        pltpu.make_async_copy(sent, sent, rep_send.at[p]).wait()

        if not last:
            start_gather(1 - p)

    for h in range(HOPS):
        hop(h % 2, h == HOPS - 1)


def local(adjacency_tiles, col_block, label_prior, seed_label, seed_mask):
    blocks_dev, degree, block_rows, _ = adjacency_tiles.shape
    nodes, classes = label_prior.shape
    n_rows = lax.axis_size("rows")
    n_cols = lax.axis_size("cols")
    group = n_cols * blocks_dev
    padded = -(-n_rows // LANES) * LANES
    pairs = max(n_cols // 2 if n_cols % 2 == 0 else n_cols, 2)
    unit = block_rows // sum(CHUNK_PARTS)
    block_bytes = 2 * block_rows * classes
    held = (2 * (group + n_rows) + 3 * n_rows) * block_bytes
    held += 2 * adjacency_tiles.size + 3 * 4 * nodes * classes
    dma = pltpu.SemaphoreType.DMA
    vmem = pl.BlockSpec(memory_space=pltpu.VMEM)
    return pl.pallas_call(
        functools.partial(kernel, n_rows, n_cols, blocks_dev, degree, block_rows, classes),
        out_shape=jax.ShapeDtypeStruct((nodes, classes), jnp.float32),
        in_specs=[
            pl.BlockSpec(memory_space=pltpu.SMEM),
            vmem,
            vmem,
            vmem,
            pl.BlockSpec(memory_space=pltpu.HBM),
        ],
        out_specs=vmem,
        scratch_shapes=[
            [
                [
                    pltpu.VMEM((group + n_rows, unit * part, classes), jnp.bfloat16)
                    for part in CHUNK_PARTS
                ]
                for _ in range(2)
            ],
            pltpu.VMEM((2, n_rows, block_rows, classes), jnp.bfloat16),
            pltpu.VMEM((n_rows, block_rows, classes), jnp.bfloat16),
            pltpu.VMEM(adjacency_tiles.shape, jnp.bfloat16),
            pltpu.VMEM((nodes, classes), jnp.float32),
            pltpu.SMEM((blocks_dev * degree,), jnp.int32),
            pltpu.VMEM((1, padded), jnp.int32),
            pltpu.VMEM((n_rows, 1, padded), jnp.int32),
            pltpu.SMEM((n_rows, 1, padded), jnp.int32),
            dma, dma, dma, dma,
            dma((2, CHUNKS)), dma((2, CHUNKS)),
            dma((2, pairs - 1, CHUNKS)), dma((2, pairs - 1, CHUNKS)),
            dma((2, pairs - 1, CHUNKS)), dma((2, pairs - 1, CHUNKS)),
            dma((2,)), dma((2,)),
        ],
        compiler_params=pltpu.CompilerParams(
            collective_id=0, has_side_effects=True, vmem_limit_bytes=held + 6 * 1024 * 1024
        ),
    )(
        col_block,
        label_prior,
        seed_label.reshape(blocks_dev, block_rows),
        seed_mask.reshape(blocks_dev, block_rows),
        adjacency_tiles,
    )


def solution(mesh):
    in_specs = (
        P(("rows", "cols"), None, None, None),
        P(("rows", "cols"), None),
        P(("rows", "cols"), None),
        P(("rows", "cols")),
        P(("rows", "cols")),
    )
    out_specs = P(("rows", "cols"), None)
    return jax.shard_map(local, mesh=mesh, in_specs=in_specs, out_specs=out_specs, check_vma=False)
```
